32 devices in a mesh: lat: 8 (over y, x, core), lon: 4 (over z).
Axes of the slice: x: 2, y: 2, z: 4, core: 2. Of those that a mesh axis runs over, the one named last changes fastest.
Arguments:
- velocity: bfloat16 [16, 1024, 512], P(None, 'lat', 'lon'), may hold values from -6 to 6
- theta: bfloat16 [16, 1024, 512], P(None, 'lat', 'lon'), may hold values from -6 to 6
- dx_cell: float32 [1024, 512], P('lat', 'lon'), may hold values from 0.5 to 2
- wet_levels: int32 [1024, 512], P('lat', 'lon'), may hold values from 0 to 16
- bottom_index: int32 [1024, 512], P('lat', 'lon'), may hold values from 1 to 4
- basin_id: int32 [1024, 512], P('lat', 'lon'), may hold values from 0 to 9
- layer_dz: float32 [16], replicated, may hold values from 0.5 to 2
Outputs:
- overturning: float32 [2, 10, 16, 1024], P(None, None, 'lon', 'lat')
The draws below stay inside these ranges and needn't reach their ends.
All inputs are finite; a program needn't handle non-finite values.
Results may differ from the reference program's by a relative error of at most 0.0003.
Values sent between devices are 32-bit elements; how exact they have to be, the bound alone decides.
A program may use at most 64 MiB of HBM per device.

```python
import math
import jax
import jax.numpy as jnp
from jax import lax

BASINS = 10
NY = 1024
NX = 512
LEV = 16


def set_ends(array, stream_key, low, largest):
    longest = array.shape.index(max(array.shape))
    spots = []
    for shift in (0, 1):
        where = [jax.random.randint(jax.random.fold_in(stream_key, axis), (), 0, length) for axis, length in enumerate(array.shape)]
        where[longest] = (where[longest] + shift) % array.shape[longest]
        spots.append(tuple(where))
    return array.at[spots[0]].set(low).at[spots[1]].set(largest)


def raised(entries, rng, source, target, blocks, factor):
    def block_of(position):
        return (jnp.arange(entries.shape[position]) // (entries.shape[position] // blocks)).reshape((-1,) + (1,) * (entries.ndim - 1 - position))

    near = jax.random.permutation(rng, blocks)[block_of(target)]
    other_side = (block_of(target) + blocks // 2) % blocks
    return jnp.where((block_of(source) == near) | (block_of(source) == other_side), factor * entries, entries)


def shard_levels(key, extent, pieces, smallest, top_value):
    loudness, own = 1.0, jax.random.fold_in(key, 6)
    for position, parts in pieces:
        draws = jnp.exp(jax.random.uniform(jax.random.fold_in(own, position), (parts,), jnp.float32, smallest / len(pieces), top_value / len(pieces)))
        loudness = loudness * jnp.repeat(draws, extent[position] // parts).reshape([-1 if axis == position else 1 for axis in range(len(extent))])
    return loudness


def bell_draw(stream_key, dims, scale, bound, shards=(), kind=jnp.bfloat16):
    values = jax.random.normal(stream_key, dims, jnp.float32) * scale
    if len(shards) > 0:
        values = shard_levels(stream_key, dims, shards, -0.22, 0.18) * values
    return jnp.clip(values, min=-bound, max=bound).astype(kind)


def gaussian_with(stream_key, shape, width, most, shards, heavy, kind=jnp.bfloat16):
    entries = width * jax.random.normal(stream_key, shape, jnp.float32)
    if shards:
        entries = entries * shard_levels(stream_key, shape, shards, -0.22, 0.18)
    return jnp.clip(raised(entries, jax.random.fold_in(stream_key, 3), *heavy), -most, most).astype(kind)


def setup_inputs(seed: int = 0) -> dict:
    seeds = jax.random.split(jax.random.key(seed), 8)
    velocity = gaussian_with(seeds[0], (LEV, NY, NX), 1.0, 6.0, ((1, 8), (2, 4)), (2, 0, 4, 2.0))
    theta = bell_draw(seeds[1], (LEV, NY, NX), 1.0, 6.0, ((1, 8), (2, 4)))
    dx_cell = jnp.clip(jnp.exp(math.log(2.0) - 1.3862944 * jax.random.uniform(seeds[2], (NY, NX), jnp.float32) ** shard_levels(seeds[2], (NY, NX), ((0, 8), (1, 4)), -0.2, 0.2)), 0.5, 2.0)
    wet_levels = set_ends(jax.random.randint(seeds[3], (NY, NX), 0, LEV + 1), jax.random.fold_in(seeds[3], 1), 0, LEV).astype(jnp.int32)
    bottom_index = set_ends(jax.random.randint(seeds[4], (NY, NX), 1, 5), jax.random.fold_in(seeds[4], 1), 1, 4).astype(jnp.int32)
    basin_id = set_ends(jax.random.randint(seeds[5], (NY, NX), 0, BASINS), jax.random.fold_in(seeds[5], 1), 0, BASINS - 1).astype(jnp.int32)
    layer_dz = jnp.clip(jnp.exp(jax.random.uniform(seeds[6], (LEV,), jnp.float32, math.log(0.5), math.log(2.0))), 0.5, 2.0)
    return {"velocity": velocity, "theta": theta, "dx_cell": dx_cell, "wet_levels": wet_levels, "bottom_index": bottom_index, "basin_id": basin_id, "layer_dz": layer_dz}


def reference(velocity, theta, dx_cell, wet_levels, bottom_index, basin_id, layer_dz):
    bottom_part = bottom_index.astype(jnp.float32) * 0.25

    def one_level(items):
        level, velocity_level, theta_level, thick_top = items
        wet_cells = (level < wet_levels).astype(jnp.float32)
        bottom_cells = level == wet_levels - 1
        thick = thick_top * jnp.where(bottom_cells, bottom_part, jnp.float32(1.0)) * wet_cells
        volume = velocity_level.astype(jnp.float32) * thick * dx_cell
        heat = volume * theta_level.astype(jnp.float32)
        vol_rows = jnp.stack([jnp.sum(jnp.where(basin_id == basin, volume, jnp.float32(0.0)), axis=1) for basin in range(BASINS)])
        heat_rows = jnp.stack([jnp.sum(jnp.where(basin_id == basin, heat, jnp.float32(0.0)), axis=1) for basin in range(BASINS)])
        return jnp.stack([vol_rows, heat_rows])

    levels = jnp.arange(LEV, dtype=jnp.int32)
    zonal = lax.map(one_level, (levels, velocity, theta, layer_dz))
    cumulated = jnp.cumsum(zonal, axis=0) * jnp.float32(1.0 / (NX ** 0.5))
    return jnp.transpose(cumulated, (1, 2, 0, 3))
```

```python
import functools

import jax
import jax.numpy as jnp
from jax import lax
from jax.experimental import pallas as pl
from jax.experimental.pallas import tpu as pltpu
from jax.sharding import PartitionSpec as P

BASINS = 10
SUB = 8


def diagonal(parts, row, lane_row):
    half = len(parts) // 2
    while half >= 1:
        low = (lane_row & half) == 0
        stay = ((row & half) == 0) == low
        merged = []
        for j in range(half):
            kept = jnp.where(low, parts[j], parts[j + half])
            moved = jnp.where(low, parts[j + half], parts[j])
            merged.append(jnp.where(stay, kept, rolled(moved, half, row)))
        parts = merged
        half //= 2
    return parts[0]


def rolled(value, half, row):
    if half == SUB // 2:
        return pltpu.roll(value, half, 0)
    up = pltpu.roll(value, half, 0)
    down = pltpu.roll(value, SUB - half, 0)
    return jnp.where((row & half) == 0, down, up)


def kernel(n, per, dz_ref, v_hbm, t_hbm, dx_hbm, wet_hbm, bot_hbm, bas_hbm, out_ref,
           v_ref, t_ref, dx_ref, wet_ref, bot_ref, bas_ref, onehot, send, recv,
           plane_sem, level_sem, send_sem, recv_sem):
    me = lax.axis_index("lon")
    ny, nx = dx_ref.shape
    groups = ny // SUB
    blocks = nx // SUB
    rows = 2 * per

    planes = [
        pltpu.make_async_copy(src, dst, plane_sem.at[i])
        for i, (src, dst) in enumerate(
            ((bas_hbm, bas_ref), (dx_hbm, dx_ref), (wet_hbm, wet_ref), (bot_hbm, bot_ref))
        )
    ]

    def level_copy(d, i):
        src, dst = ((v_hbm, v_ref), (t_hbm, t_ref))[i]
        part = pl.ds(d * per, per)
        return pltpu.make_async_copy(src.at[part], dst.at[part], level_sem.at[d, i])

    for copy in planes:
        copy.start()
    for d in range(n):
        level_copy(d, 0).start()
        level_copy(d, 1).start()

    barrier = pltpu.get_barrier_semaphore()
    for off in range(1, n):
        pl.semaphore_signal(
            barrier, inc=1, device_id={"lon": lax.rem(me + off, n)}, device_id_type=pl.DeviceIdType.MESH
        )

    row = lax.broadcasted_iota(jnp.int32, (SUB, nx), 0)
    lane = lax.broadcasted_iota(jnp.int32, (SUB, nx), 1)
    lane_row = lane % SUB
    lane_block = lane // SUB
    level_row = row % per

    planes[0].wait()
    for g in range(groups):
        basin = bas_ref[g * SUB:(g + 1) * SUB, :]
        hot = jnp.concatenate(
            [(basin == (p - g) % blocks).astype(jnp.float32) for p in range(blocks)], axis=0
        )
        onehot[g] = hot.astype(jnp.bfloat16)
    for copy in planes[1:]:
        copy.wait()
    bot_scale = 0.25

    def remote(d, slot):
        return pltpu.make_async_remote_copy(
            src_ref=send.at[d],
            dst_ref=recv.at[slot],
            send_sem=send_sem.at[d],
            recv_sem=recv_sem.at[slot],
            device_id={"lon": d},
            device_id_type=pl.DeviceIdType.MESH,
        )

    def one_group(d, carry):
        level_copy(d, 0).wait()
        level_copy(d, 1).wait()
        first = d * per
        merged = [jnp.zeros((SUB, nx), jnp.float32)] * BASINS
        for pair in range(groups // 2):
            both = slice(pair * 2 * SUB, (pair + 1) * 2 * SUB)
            v_both = v_ref[pl.ds(first, per), both, :].astype(jnp.float32)
            t_both = t_ref[pl.ds(first, per), both, :].astype(jnp.float32)
            for side in range(2):
                g = pair * 2 + side
                span = slice(g * SUB, (g + 1) * SUB)
                part = slice(side * SUB, (side + 1) * SUB)
                dx = dx_ref[span, :]
                last = wet_ref[span, :] - 1
                dx_last = dx * (bot_ref[span, :].astype(jnp.float32) * bot_scale)
                volumes, heats = [], []
                for k in range(per):
                    width = jnp.where(
                        first + k < last, dx, jnp.where(first + k == last, dx_last, jnp.float32(0.0))
                    )
                    volume = v_both[k, part, :] * width
                    volumes.append(volume)
                    heats.append(volume * t_both[k, part, :])
                values = jnp.concatenate(volumes + heats, axis=0)
                high = values.astype(jnp.bfloat16)
                low = (values - high.astype(jnp.float32)).astype(jnp.bfloat16)
                hot = onehot[g]
                sums = lax.dot_general(
                    jnp.concatenate([high, low], axis=1),
                    jnp.concatenate([hot, hot], axis=1),
                    (((1,), (1,)), ((), ())),
                    preferred_element_type=jnp.float32,
                )
                picked = diagonal([sums[j * SUB:(j + 1) * SUB, :] for j in range(rows)], row, lane_row)
                merged = [
                    jnp.where(lane_block == (g + b) % blocks, picked, merged[b]) for b in range(BASINS)
                ]
        dz = dz_ref[first]
        for k in range(1, per):
            dz = jnp.where(level_row == k, dz_ref[first + k], dz)
        following = []
        for b in range(BASINS):
            total = merged[b] if b == 0 else pltpu.roll(merged[b], nx - b * SUB, 1)
            total = total * dz
            step = 1
            while step < per:
                total = total + jnp.where(level_row >= step, pltpu.roll(total, step, 0), jnp.float32(0.0))
                step *= 2
            total = total + carry[b]
            send[d, b] = total
            following.append(
                jnp.where(
                    row < per,
                    jnp.broadcast_to(total[per - 1:per, :], total.shape),
                    jnp.broadcast_to(total[2 * per - 1:2 * per, :], total.shape),
                )
            )
        if isinstance(d, int):
            if d == 0:
                pl.semaphore_wait(barrier, n - 1)
        else:
            @pl.when(d == 0)
            def _():
                pl.semaphore_wait(barrier, n - 1)

        @pl.when(d != me)
        def _():
            remote(d, me).start()

        return tuple(following)

    zero = tuple(jnp.zeros((SUB, nx), jnp.float32) for _ in range(BASINS))
    lax.fori_loop(0, n, one_group, zero)

    for off in range(1, n):
        remote(lax.rem(me + off, n), me).wait_send()
    total = send[me]
    for off in range(1, n):
        source = lax.rem(me + off, n)
        remote(source, source).wait_recv()
        total = total + recv[source]
    out_ref[...] = total * jnp.float32(1.0 / (nx * n) ** 0.5)


def solution(mesh):
    n = mesh.shape["lon"]

    def on_device(velocity, theta, dx_cell, wet_levels, bottom_index, basin_id, layer_dz):
        levels, ny, nx = velocity.shape
        per = levels // n
        assert 2 * per == SUB and ny == nx and BASINS * SUB <= nx
        anywhere = pl.BlockSpec(memory_space=pl.ANY)
        piece = (BASINS, 2 * per, nx)
        result = pl.pallas_call(
            functools.partial(kernel, n, per),
            out_shape=jax.ShapeDtypeStruct(piece, jnp.float32),
            in_specs=[pl.BlockSpec(memory_space=pltpu.SMEM)] + [anywhere] * 6,
            out_specs=pl.BlockSpec(memory_space=pltpu.VMEM),
            scratch_shapes=[
                pltpu.VMEM((levels, ny, nx), jnp.bfloat16),
                pltpu.VMEM((levels, ny, nx), jnp.bfloat16),
                pltpu.VMEM((ny, nx), jnp.float32),
                pltpu.VMEM((ny, nx), jnp.int32),
                pltpu.VMEM((ny, nx), jnp.int32),
                pltpu.VMEM((ny, nx), jnp.int32),
                pltpu.VMEM((ny // SUB, nx, nx), jnp.bfloat16),
                pltpu.VMEM((n, *piece), jnp.float32),
                pltpu.VMEM((n, *piece), jnp.float32),
                pltpu.SemaphoreType.DMA((4,)),
                pltpu.SemaphoreType.DMA((n, 2)),
                pltpu.SemaphoreType.DMA((n,)),
                pltpu.SemaphoreType.DMA((n,)),
            ],
            compiler_params=pltpu.CompilerParams(collective_id=0, has_side_effects=True),
        )(layer_dz, velocity, theta, dx_cell, wet_levels, bottom_index, basin_id)
        return jnp.transpose(result.reshape(BASINS, 2, per, ny), (1, 0, 2, 3))

    placed = (
        P(None, "lat", "lon"),
        P(None, "lat", "lon"),
        P("lat", "lon"),
        P("lat", "lon"),
        P("lat", "lon"),
        P("lat", "lon"),
        P(),
    )
    return jax.shard_map(
        on_device,
        mesh=mesh,
        in_specs=placed,
        out_specs=P(None, None, "lon", "lat"),
        check_vma=False,
    )
```

```python
import functools

import jax
import jax.numpy as jnp
from jax import lax
from jax.experimental import pallas as pl
from jax.experimental.pallas import tpu as pltpu
from jax.sharding import PartitionSpec as P

BASINS = 10
SUB = 8


def diagonal(parts, row, lane_row):
    half = len(parts) // 2
    while half >= 1:
        low = (lane_row & half) == 0
        stay = ((row & half) == 0) == low
        merged = []
        for j in range(half):
            kept = jnp.where(low, parts[j], parts[j + half])
            moved = jnp.where(low, parts[j + half], parts[j])
            merged.append(jnp.where(stay, kept, rolled(moved, half, row)))
        parts = merged
        half //= 2
    return parts[0]


def rolled(value, half, row):
    if half == SUB // 2:
        return pltpu.roll(value, half, 0)
    up = pltpu.roll(value, half, 0)
    down = pltpu.roll(value, SUB - half, 0)
    return jnp.where((row & half) == 0, down, up)


def kernel(n, per, dz_ref, v_hbm, t_hbm, dx_hbm, wet_hbm, bot_hbm, bas_hbm, out_ref,
           v_ref, t_ref, dx_ref, wet_ref, bot_ref, bas_ref, onehot, send, recv,
           plane_sem, level_sem, send_sem, recv_sem):
    me = lax.axis_index("lon")
    ny, nx = dx_ref.shape
    groups = ny // SUB
    blocks = nx // SUB
    rows = 2 * per

    planes = [
        pltpu.make_async_copy(src, dst, plane_sem.at[i])
        for i, (src, dst) in enumerate(
            ((bas_hbm, bas_ref), (dx_hbm, dx_ref), (wet_hbm, wet_ref), (bot_hbm, bot_ref))
        )
    ]

    def level_copy(d, i):
        src, dst = ((v_hbm, v_ref), (t_hbm, t_ref))[i]
        part = pl.ds(d * per, per)
        return pltpu.make_async_copy(src.at[part], dst.at[part], level_sem.at[d, i])

    for copy in planes:
        copy.start()
    for d in range(n):
        level_copy(d, 0).start()
        level_copy(d, 1).start()

    barrier = pltpu.get_barrier_semaphore()
    for off in range(1, n):
        pl.semaphore_signal(
            barrier, inc=1, device_id={"lon": lax.rem(me + off, n)}, device_id_type=pl.DeviceIdType.MESH
        )

    row = lax.broadcasted_iota(jnp.int32, (SUB, nx), 0)
    lane = lax.broadcasted_iota(jnp.int32, (SUB, nx), 1)
    lane_row = lane % SUB
    lane_block = lane // SUB
    level_row = row % per

    planes[0].wait()
    for g in range(groups):
        basin = bas_ref[g * SUB:(g + 1) * SUB, :]
        hot = jnp.concatenate(
            [(basin == (p - g) % blocks).astype(jnp.float32) for p in range(blocks)], axis=0
        )
        onehot[g] = hot.astype(jnp.bfloat16)
    for copy in planes[1:]:
        copy.wait()
    bot_scale = 0.25

    def remote(d, slot):
        return pltpu.make_async_remote_copy(
            src_ref=send.at[d],
            dst_ref=recv.at[slot],
            send_sem=send_sem.at[d],
            recv_sem=recv_sem.at[slot],
            device_id={"lon": d},
            device_id_type=pl.DeviceIdType.MESH,
        )

    def one_group(d, carry):
        level_copy(d, 0).wait()
        level_copy(d, 1).wait()
        first = d * per
        merged = [jnp.zeros((SUB, nx), jnp.float32)] * BASINS
        for pair in range(groups // 2):
            both = slice(pair * 2 * SUB, (pair + 1) * 2 * SUB)
            v_both = v_ref[pl.ds(first, per), both, :].astype(jnp.float32)
            t_both = t_ref[pl.ds(first, per), both, :].astype(jnp.float32)
            for side in range(2):
                g = pair * 2 + side
                span = slice(g * SUB, (g + 1) * SUB)
                part = slice(side * SUB, (side + 1) * SUB)
                dx = dx_ref[span, :]
                last = wet_ref[span, :] - 1
                dx_last = dx * (bot_ref[span, :].astype(jnp.float32) * bot_scale)
                volumes, heats = [], []
                for k in range(per):
                    width = jnp.where(
                        first + k < last, dx, jnp.where(first + k == last, dx_last, jnp.float32(0.0))
                    )
                    volume = v_both[k, part, :] * width
                    volumes.append(volume)
                    heats.append(volume * t_both[k, part, :])
                values = jnp.concatenate(volumes + heats, axis=0)
                high = values.astype(jnp.bfloat16)
                low = (values - high.astype(jnp.float32)).astype(jnp.bfloat16)
                hot = onehot[g]
                sums = lax.dot_general(
                    jnp.concatenate([high, low], axis=1),
                    jnp.concatenate([hot, hot], axis=1),
                    (((1,), (1,)), ((), ())),
                    preferred_element_type=jnp.float32,
                )
                picked = diagonal([sums[j * SUB:(j + 1) * SUB, :] for j in range(rows)], row, lane_row)
                merged = [
                    jnp.where(lane_block == (g + b) % blocks, picked, merged[b]) for b in range(BASINS)
                ]
        dz = dz_ref[first]
        for k in range(1, per):
            dz = jnp.where(level_row == k, dz_ref[first + k], dz)
        following = []
        for b in range(BASINS):
            total = merged[b] if b == 0 else pltpu.roll(merged[b], nx - b * SUB, 1)
            total = total * dz
            step = 1
            while step < per:
                total = total + jnp.where(level_row >= step, pltpu.roll(total, step, 0), jnp.float32(0.0))
                step *= 2
            total = total + carry[b]
            send[d, b] = total
            following.append(
                jnp.where(
                    row < per,
                    jnp.broadcast_to(total[per - 1:per, :], total.shape),
                    jnp.broadcast_to(total[2 * per - 1:2 * per, :], total.shape),
                )
            )
        if isinstance(d, int):
            if d == 0:
                pl.semaphore_wait(barrier, n - 1)
        else:
            @pl.when(d == 0)
            def _():
                pl.semaphore_wait(barrier, n - 1)

        @pl.when(d != me)
        def _():
            remote(d, me).start()

        return tuple(following)

    zero = tuple(jnp.zeros((SUB, nx), jnp.float32) for _ in range(BASINS))
    lax.fori_loop(0, n, one_group, zero)

    for off in range(1, n):
        remote(lax.rem(me + off, n), me).wait_send()
    total = send[me]
    for off in range(1, n):
        source = lax.rem(me + off, n)
        remote(source, source).wait_recv()
        total = total + recv[source]
    out_ref[...] = total * jnp.float32(1.0 / (nx * n) ** 0.5)


def solution(mesh):
    n = mesh.shape["lon"]

    def on_device(velocity, theta, dx_cell, wet_levels, bottom_index, basin_id, layer_dz):
        levels, ny, nx = velocity.shape
        per = levels // n
        assert 2 * per == SUB and ny == nx and BASINS * SUB <= nx
        anywhere = pl.BlockSpec(memory_space=pl.ANY)
        piece = (BASINS, 2 * per, nx)
        result = pl.pallas_call(
            functools.partial(kernel, n, per),
            out_shape=pltpu.VMEM(piece, jnp.float32),
            in_specs=[pl.BlockSpec(memory_space=pltpu.SMEM)] + [anywhere] * 6,
            out_specs=pl.BlockSpec(memory_space=pltpu.VMEM),
            scratch_shapes=[
                pltpu.VMEM((levels, ny, nx), jnp.bfloat16),
                pltpu.VMEM((levels, ny, nx), jnp.bfloat16),
                pltpu.VMEM((ny, nx), jnp.float32),
                pltpu.VMEM((ny, nx), jnp.int32),
                pltpu.VMEM((ny, nx), jnp.int32),
                pltpu.VMEM((ny, nx), jnp.int32),
                pltpu.VMEM((ny // SUB, nx, nx), jnp.bfloat16),
                pltpu.VMEM((n, *piece), jnp.float32),
                pltpu.VMEM((n, *piece), jnp.float32),
                pltpu.SemaphoreType.DMA((4,)),
                pltpu.SemaphoreType.DMA((n, 2)),
                pltpu.SemaphoreType.DMA((n,)),
                pltpu.SemaphoreType.DMA((n,)),
            ],
            compiler_params=pltpu.CompilerParams(collective_id=0, has_side_effects=True),
        )(layer_dz, velocity, theta, dx_cell, wet_levels, bottom_index, basin_id)
        return jnp.transpose(result.reshape(BASINS, 2, per, ny), (1, 0, 2, 3))

    placed = (
        P(None, "lat", "lon"),
        P(None, "lat", "lon"),
        P("lat", "lon"),
        P("lat", "lon"),
        P("lat", "lon"),
        P("lat", "lon"),
        P(),
    )
    return jax.shard_map(
        on_device,
        mesh=mesh,
        in_specs=placed,
        out_specs=P(None, None, "lon", "lat"),
        check_vma=False,
    )
```

```python
import functools

import jax
import jax.numpy as jnp
from jax import lax
from jax.experimental import pallas as pl
from jax.experimental.pallas import tpu as pltpu
from jax.sharding import PartitionSpec as P

BASINS = 10
SUB = 8
CHUNKS = 4


def choose(parts, spot):
    bit = 1
    while len(parts) > 1:
        odd = (spot & bit) != 0
        parts = [jnp.where(odd, parts[j + 1], parts[j]) for j in range(0, len(parts), 2)]
        bit *= 2
    return parts[0]


def kernel(n, per, dz_ref, v_hbm, t_hbm, dx_hbm, wet_hbm, bot_hbm, bas_hbm, out_ref,
           v_ref, t_ref, dx_ref, wet_ref, bot_ref, bas_ref, picked, send, recv,
           chunk_sem, send_sem, recv_sem):
    me = lax.axis_index("lon")
    ny, nx = dx_ref.shape
    groups = ny // SUB
    blocks = nx // SUB
    rows = 2 * per
    chunk_rows = ny // CHUNKS

    def chunk(c):
        span = pl.ds(c * chunk_rows, chunk_rows)
        pairs = [(bas_hbm, bas_ref), (dx_hbm, dx_ref), (wet_hbm, wet_ref), (bot_hbm, bot_ref)]
        views = [(src.at[span], dst.at[span]) for src, dst in pairs]
        views += [(src.at[:, span], dst.at[:, span]) for src, dst in ((v_hbm, v_ref), (t_hbm, t_ref))]
        return [pltpu.make_async_copy(src, dst, chunk_sem.at[c, i]) for i, (src, dst) in enumerate(views)]

    for c in range(CHUNKS):
        for copy in chunk(c):
            copy.start()

    barrier = pltpu.get_barrier_semaphore()
    for off in range(1, n):
        pl.semaphore_signal(
            barrier, inc=1, device_id={"lon": lax.rem(me + off, n)}, device_id_type=pl.DeviceIdType.MESH
        )

    row = lax.broadcasted_iota(jnp.int32, (SUB, nx), 0)
    lane = lax.broadcasted_iota(jnp.int32, (SUB, nx), 1)
    lane_block = lane // SUB
    level_row = row % per
    source_part = (row - lane) % SUB

    def sums_of(g, v_both, t_both, side, first_level):
        span = slice(g * SUB, (g + 1) * SUB)
        part = slice(side * SUB, (side + 1) * SUB)
        basin = (bas_ref[span, :] + g) % blocks
        hot = jnp.concatenate([(basin == p).astype(jnp.float32) for p in range(blocks)], axis=0)
        hot = hot.astype(jnp.bfloat16)
        dx = dx_ref[span, :]
        last = wet_ref[span, :] - 1
        dx_last = dx * (bot_ref[span, :].astype(jnp.float32) * 0.25)
        tiles = []
        sets = v_both.shape[0] // per
        for s in range(sets):
            volumes, heats = [], []
            for k in range(per):
                level = first_level + s * per + k
                width = jnp.where(level < last, dx, jnp.where(level == last, dx_last, jnp.float32(0.0)))
                volume = v_both[s * per + k, part, :] * width
                heat = volume * t_both[s * per + k, part, :]
                volumes.append(volume if k == 0 else pltpu.roll(volume, k, 0))
                heats.append(pltpu.roll(heat, per + k, 0))
            tiles += volumes + heats
        values = jnp.concatenate(tiles, axis=0)
        high = values.astype(jnp.bfloat16)
        low = (values - high.astype(jnp.float32)).astype(jnp.bfloat16)
        out = lax.dot_general(
            jnp.concatenate([high, low], axis=1),
            jnp.concatenate([hot, hot], axis=1),
            (((1,), (1,)), ((), ())),
            preferred_element_type=jnp.float32,
        )
        for s in range(sets):
            base = s * rows * SUB
            parts = [out[base + j * SUB:base + (j + 1) * SUB, :] for j in range(rows)]
            picked[first_level // per + s, g] = choose(parts, source_part)

    most = 4 * per
    for c in range(CHUNKS):
        for copy in chunk(c):
            copy.wait()
        for pair in range(chunk_rows // (2 * SUB)):
            begin = c * chunk_rows + pair * 2 * SUB
            both = slice(begin, begin + 2 * SUB)
            for first_level in range(0, n * per, most):
                held = slice(first_level, min(first_level + most, n * per))
                v_both = v_ref[held, both, :].astype(jnp.float32)
                t_both = t_ref[held, both, :].astype(jnp.float32)
                for side in range(2):
                    sums_of(begin // SUB + side, v_both, t_both, side, first_level)

    def remote(d, slot):
        return pltpu.make_async_remote_copy(
            src_ref=send.at[d],
            dst_ref=recv.at[slot],
            send_sem=send_sem.at[d],
            recv_sem=recv_sem.at[slot],
            device_id={"lon": d},
            device_id_type=pl.DeviceIdType.MESH,
        )

    scale = 1.0 / (nx * n) ** 0.5

    def cumulate(d, carry):
        tiles = [picked[d, g] for g in range(groups)]
        dz = dz_ref[d * per]
        for k in range(1, per):
            dz = jnp.where(level_row == k, dz_ref[d * per + k], dz)
        dz = dz * jnp.float32(scale)
        following = []
        for b in range(BASINS):
            total = tiles[0]
            for g in range(1, groups):
                total = jnp.where(lane_block == (g + b) % blocks, tiles[g], total)
            if b:
                total = pltpu.roll(total, nx - b * SUB, 1)
            shift = 1
            while shift < SUB:
                total = jnp.where((lane & shift) != 0, pltpu.roll(total, SUB - shift, 0), total)
                shift *= 2
            total = total * dz
            step = 1
            while step < per:
                total = total + jnp.where(level_row >= step, pltpu.roll(total, step, 0), jnp.float32(0.0))
                step *= 2
            total = total + carry[b]
            send[d, b] = total
            following.append(
                jnp.where(
                    row < per,
                    jnp.broadcast_to(total[per - 1:per, :], total.shape),
                    jnp.broadcast_to(total[2 * per - 1:2 * per, :], total.shape),
                )
            )
        return tuple(following)

    carry = tuple(jnp.zeros((SUB, nx), jnp.float32) for _ in range(BASINS))
    if n <= 4:
        for d in range(n):
            carry = cumulate(d, carry)
    else:
        lax.fori_loop(0, n, cumulate, carry)

    pl.semaphore_wait(barrier, n - 1)
    for off in range(n - 1, 0, -1):
        for target in (me + off, me - off):

            @pl.when((target >= 0) & (target < n))
            def _():
                remote(target, me).start()

    total = send[me]
    for off in range(1, n):
        source = lax.rem(me + off, n)
        remote(source, source).wait_recv()
        total = total + recv[source]
    out_ref[...] = total
    for off in range(1, n):
        remote(lax.rem(me + off, n), me).wait_send()


def solution(mesh):
    n = mesh.shape["lon"]

    def on_device(velocity, theta, dx_cell, wet_levels, bottom_index, basin_id, layer_dz):
        levels, ny, nx = velocity.shape
        per = levels // n
        assert 2 * per == SUB and ny == nx and BASINS * SUB <= nx
        anywhere = pl.BlockSpec(memory_space=pl.ANY)
        piece = (BASINS, 2 * per, nx)
        result = pl.pallas_call(
            functools.partial(kernel, n, per),
            out_shape=pltpu.VMEM(piece, jnp.float32),
            in_specs=[pl.BlockSpec(memory_space=pltpu.SMEM)] + [anywhere] * 6,
            out_specs=pl.BlockSpec(memory_space=pltpu.VMEM),
            scratch_shapes=[
                pltpu.VMEM((levels, ny, nx), jnp.bfloat16),
                pltpu.VMEM((levels, ny, nx), jnp.bfloat16),
                pltpu.VMEM((ny, nx), jnp.float32),
                pltpu.VMEM((ny, nx), jnp.int32),
                pltpu.VMEM((ny, nx), jnp.int32),
                pltpu.VMEM((ny, nx), jnp.int32),
                pltpu.VMEM((n, ny // SUB, SUB, nx), jnp.float32),
                pltpu.VMEM((n, *piece), jnp.float32),
                pltpu.VMEM((n, *piece), jnp.float32),
                pltpu.SemaphoreType.DMA((CHUNKS, 6)),
                pltpu.SemaphoreType.DMA((n,)),
                pltpu.SemaphoreType.DMA((n,)),
            ],
            compiler_params=pltpu.CompilerParams(collective_id=0, has_side_effects=True),
        )(layer_dz, velocity, theta, dx_cell, wet_levels, bottom_index, basin_id)
        return jnp.transpose(result.reshape(BASINS, 2, per, ny), (1, 0, 2, 3))

    placed = (
        P(None, "lat", "lon"),
        P(None, "lat", "lon"),
        P("lat", "lon"),
        P("lat", "lon"),
        P("lat", "lon"),
        P("lat", "lon"),
        P(),
    )
    return jax.shard_map(
        on_device,
        mesh=mesh,
        in_specs=placed,
        out_specs=P(None, None, "lon", "lat"),
        check_vma=False,
    )
```

```python
import functools

import jax
import jax.numpy as jnp
from jax import lax
from jax.experimental import pallas as pl
from jax.experimental.pallas import tpu as pltpu
from jax.sharding import PartitionSpec as P

BASINS = 10
SUB = 8


def choose(parts, spot):
    bit = 1
    while len(parts) > 1:
        odd = (spot & bit) != 0
        parts = [jnp.where(odd, parts[j + 1], parts[j]) for j in range(0, len(parts), 2)]
        bit *= 2
    return parts[0]


def kernel(n, per, dz_hbm, v_hbm, t_hbm, dx_hbm, wet_hbm, bot_hbm, bas_hbm, out_ref,
           dz_ref, v_ref, t_ref, dx_ref, wet_ref, bot_ref, bas_ref, onehot, send, recv,
           plane_sem, level_sem, send_sem, recv_sem):
    me = lax.axis_index("lon")
    ny, nx = dx_ref.shape
    groups = ny // SUB
    blocks = nx // SUB
    rows = 2 * per

    planes = [
        pltpu.make_async_copy(src, dst, plane_sem.at[i])
        for i, (src, dst) in enumerate(
            ((bas_hbm, bas_ref), (dx_hbm, dx_ref), (wet_hbm, wet_ref), (bot_hbm, bot_ref), (dz_hbm, dz_ref))
        )
    ]

    def level_copy(d, i):
        src, dst = ((v_hbm, v_ref), (t_hbm, t_ref))[i]
        part = pl.ds(d * per, per)
        return pltpu.make_async_copy(src.at[part], dst.at[part], level_sem.at[d, i])

    barrier = pltpu.get_barrier_semaphore()
    for off in range(1, n):
        pl.semaphore_signal(
            barrier, inc=1, device_id={"lon": lax.rem(me + off, n)}, device_id_type=pl.DeviceIdType.MESH
        )

    for copy in planes:
        copy.start()
    for d in range(n):
        level_copy(d, 0).start()
        level_copy(d, 1).start()

    row = lax.broadcasted_iota(jnp.int32, (SUB, nx), 0)
    lane = lax.broadcasted_iota(jnp.int32, (SUB, nx), 1)
    source_part = (row - lane) % SUB
    lane_block = lane // SUB
    level_row = row % per

    planes[0].wait()
    for g in range(groups):
        basin = bas_ref[g * SUB:(g + 1) * SUB, :]
        hot = jnp.concatenate(
            [(basin == (p - g) % blocks).astype(jnp.float32) for p in range(blocks)], axis=0
        )
        onehot[g] = hot.astype(jnp.bfloat16)
    for copy in planes[1:]:
        copy.wait()
    bot_scale = 0.25

    def remote(d, slot):
        return pltpu.make_async_remote_copy(
            src_ref=send.at[d],
            dst_ref=recv.at[slot],
            send_sem=send_sem.at[d],
            recv_sem=recv_sem.at[slot],
            device_id={"lon": d},
            device_id_type=pl.DeviceIdType.MESH,
        )

    def one_group(d, carry):
        level_copy(d, 0).wait()
        level_copy(d, 1).wait()
        first = d * per
        merged = [jnp.zeros((SUB, nx), jnp.float32)] * BASINS
        for pair in range(groups // 2):
            both = slice(pair * 2 * SUB, (pair + 1) * 2 * SUB)
            v_both = v_ref[pl.ds(first, per), both, :].astype(jnp.float32)
            t_both = t_ref[pl.ds(first, per), both, :].astype(jnp.float32)
            for side in range(2):
                g = pair * 2 + side
                span = slice(g * SUB, (g + 1) * SUB)
                part = slice(side * SUB, (side + 1) * SUB)
                dx = dx_ref[span, :]
                last = wet_ref[span, :] - 1
                dx_last = dx * (bot_ref[span, :].astype(jnp.float32) * bot_scale)
                volumes, heats = [], []
                for k in range(per):
                    width = jnp.where(
                        first + k < last, dx, jnp.where(first + k == last, dx_last, jnp.float32(0.0))
                    )
                    volume = v_both[k, part, :] * width
                    heat = volume * t_both[k, part, :]
                    volumes.append(volume if k == 0 else pltpu.roll(volume, k, 0))
                    heats.append(pltpu.roll(heat, per + k, 0))
                values = jnp.concatenate(volumes + heats, axis=0)
                high = values.astype(jnp.bfloat16)
                low = (values - high.astype(jnp.float32)).astype(jnp.bfloat16)
                hot = onehot[g]
                sums = lax.dot_general(
                    jnp.concatenate([high, low], axis=1),
                    jnp.concatenate([hot, hot], axis=1),
                    (((1,), (1,)), ((), ())),
                    preferred_element_type=jnp.float32,
                )
                picked = choose([sums[j * SUB:(j + 1) * SUB, :] for j in range(rows)], source_part)
                merged = [
                    jnp.where(lane_block == (g + b) % blocks, picked, merged[b]) for b in range(BASINS)
                ]
        dz = dz_ref[first]
        for k in range(1, per):
            dz = jnp.where(level_row == k, dz_ref[first + k], dz)
        dz = dz * jnp.float32(1.0 / (nx * n) ** 0.5)
        following = []
        for b in range(BASINS):
            total = merged[b] if b == 0 else pltpu.roll(merged[b], nx - b * SUB, 1)
            shift = 1
            while shift < SUB:
                total = jnp.where((lane & shift) != 0, pltpu.roll(total, SUB - shift, 0), total)
                shift *= 2
            total = total * dz
            step = 1
            while step < per:
                total = total + jnp.where(level_row >= step, pltpu.roll(total, step, 0), jnp.float32(0.0))
                step *= 2
            total = total + carry[b]
            send[d, b] = total
            following.append(
                jnp.where(
                    row < per,
                    jnp.broadcast_to(total[per - 1:per, :], total.shape),
                    jnp.broadcast_to(total[2 * per - 1:2 * per, :], total.shape),
                )
            )
        if isinstance(d, int):
            if d == 0:
                pl.semaphore_wait(barrier, n - 1)
        else:
            @pl.when(d == 0)
            def _():
                pl.semaphore_wait(barrier, n - 1)

        @pl.when(d != me)
        def _():
            remote(d, me).start()

        return tuple(following)

    zero = tuple(jnp.zeros((SUB, nx), jnp.float32) for _ in range(BASINS))
    lax.fori_loop(0, n, one_group, zero)

    total = send[me]
    for off in range(1, n):
        source = lax.rem(me + off, n)
        remote(source, source).wait_recv()
        total = total + recv[source]
    out_ref[...] = total
    for off in range(1, n):
        remote(lax.rem(me + off, n), me).wait_send()


def solution(mesh):
    n = mesh.shape["lon"]

    def on_device(velocity, theta, dx_cell, wet_levels, bottom_index, basin_id, layer_dz):
        levels, ny, nx = velocity.shape
        per = levels // n
        assert 2 * per == SUB and ny == nx and BASINS * SUB <= nx
        anywhere = pl.BlockSpec(memory_space=pl.ANY)
        piece = (BASINS, 2 * per, nx)
        result = pl.pallas_call(
            functools.partial(kernel, n, per),
            out_shape=pltpu.VMEM(piece, jnp.float32),
            in_specs=[anywhere] * 7,
            out_specs=pl.BlockSpec(memory_space=pltpu.VMEM),
            scratch_shapes=[
                pltpu.SMEM((levels,), jnp.float32),
                pltpu.VMEM((levels, ny, nx), jnp.bfloat16),
                pltpu.VMEM((levels, ny, nx), jnp.bfloat16),
                pltpu.VMEM((ny, nx), jnp.float32),
                pltpu.VMEM((ny, nx), jnp.int32),
                pltpu.VMEM((ny, nx), jnp.int32),
                pltpu.VMEM((ny, nx), jnp.int32),
                pltpu.VMEM((ny // SUB, nx, nx), jnp.bfloat16),
                pltpu.VMEM((n, *piece), jnp.float32),
                pltpu.VMEM((n, *piece), jnp.float32),
                pltpu.SemaphoreType.DMA((5,)),
                pltpu.SemaphoreType.DMA((n, 2)),
                pltpu.SemaphoreType.DMA((n,)),
                pltpu.SemaphoreType.DMA((n,)),
            ],
            compiler_params=pltpu.CompilerParams(collective_id=0, has_side_effects=True),
        )(layer_dz, velocity, theta, dx_cell, wet_levels, bottom_index, basin_id)
        return jnp.transpose(result.reshape(BASINS, 2, per, ny), (1, 0, 2, 3))

    placed = (
        P(None, "lat", "lon"),
        P(None, "lat", "lon"),
        P("lat", "lon"),
        P("lat", "lon"),
        P("lat", "lon"),
        P("lat", "lon"),
        P(),
    )
    return jax.shard_map(
        on_device,
        mesh=mesh,
        in_specs=placed,
        out_specs=P(None, None, "lon", "lat"),
        check_vma=False,
    )
```
